8 devices in a mesh: pod: 1 (over z), dp: 2 (over y), ep: 4 (over x, core).
Axes of the slice: x: 2, y: 2, z: 1, core: 2. Of those that a mesh axis runs over, the one named last changes fastest.
Arguments:
- x_start: bfloat16 [8192, 1024], P(('pod', 'dp', 'ep'))
- route_a: int32 [8192, 2], P(('pod', 'dp', 'ep'))
- route_b: int32 [8192, 2], P(('pod', 'dp', 'ep'))
- gate_a: float32 [8192, 2], P(('pod', 'dp', 'ep'))
- gate_b: float32 [8192, 2], P(('pod', 'dp', 'ep'))
- grad_out: bfloat16 [8192, 1024], P(('pod', 'dp', 'ep'))
- w1_a: bfloat16 [8, 1024, 3584], P('ep')
- w3_a: bfloat16 [8, 1024, 3584], P('ep')
- w2_a: bfloat16 [8, 3584, 1024], P('ep')
- w1_b: bfloat16 [8, 1024, 3584], P('ep')
- w3_b: bfloat16 [8, 1024, 3584], P('ep')
- w2_b: bfloat16 [8, 3584, 1024], P('ep')
Outputs:
- output 1: bfloat16 [8192, 1024], P(('pod', 'dp', 'ep'))
- output 2: bfloat16 [8192, 1024], P(('pod', 'dp', 'ep'))
- output 3: float32 [8, 1024, 3584], P(('pod', 'ep'), 'dp')
- output 4: float32 [8, 1024, 3584], P(('pod', 'ep'), 'dp')
- output 5: float32 [8, 3584, 1024], P(('pod', 'ep'), 'dp')
- output 6: float32 [8, 1024, 3584], P(('pod', 'ep'), 'dp')
- output 7: float32 [8, 1024, 3584], P(('pod', 'ep'), 'dp')
- output 8: float32 [8, 3584, 1024], P(('pod', 'ep'), 'dp')
- output 9: float32 [8192, 2], P(('pod', 'dp', 'ep'))
- output 10: float32 [8192, 2], P(('pod', 'dp', 'ep'))
All inputs are finite; a program needn't handle non-finite values.
Results may differ from the reference program's by a relative error of at most 0.00888651.
Values are sent between devices in bfloat16 or wider.
A program may use at most 1 GiB of HBM per device.

```python
import jax
import jax.numpy as jnp
from jax import lax

MODEL_DIM = 1024
FFN_DIM = 3584
EXPERTS = 8
TOP_K = 2
TOKENS_DEV = 1024
PART_DEVS = 8

CAPACITY = 3 * TOKENS_DEV * TOP_K // (2 * EXPERTS)
MEAN_LOAD = TOKENS_DEV * TOP_K // EXPERTS
PART_TOKENS = PART_DEVS * TOKENS_DEV
SLOT_ROWS = PART_DEVS * CAPACITY


def draw_routing(route_key):
    def one_device(dev_key):
        key_order, key_tokens = jax.random.split(dev_key)
        expert_order = jax.random.permutation(key_order, EXPERTS).astype(jnp.int32)
        counts = jnp.where(jnp.arange(EXPERTS) % 2 == 0, CAPACITY, 2 * MEAN_LOAD - CAPACITY)
        flat_ids = jnp.repeat(expert_order, counts, total_repeat_length=TOKENS_DEV * TOP_K)
        id_table = flat_ids.reshape(TOP_K, TOKENS_DEV).T
        return id_table[jax.random.permutation(key_tokens, TOKENS_DEV)]
    dev_keys = jax.random.split(route_key, PART_DEVS)
    return jax.vmap(one_device)(dev_keys).reshape(PART_TOKENS, TOP_K).astype(jnp.int32)


def setup_inputs(seed: int = 0, part: int = 0) -> dict:
    base_key = jax.random.key(seed)
    shared_key, group_key = jax.random.split(base_key)
    group_key = jax.random.fold_in(group_key, part)
    part_keys = jax.random.split(group_key, 6)
    weight_keys = jax.random.split(shared_key, 6)
    up_scale = MODEL_DIM ** -0.5
    down_scale = FFN_DIM ** -0.5
    gate_scale = TOP_K ** -0.5
    up_shape = (EXPERTS, MODEL_DIM, FFN_DIM)
    down_shape = (EXPERTS, FFN_DIM, MODEL_DIM)
    tok_shape = (PART_TOKENS, MODEL_DIM)
    pair_shape = (PART_TOKENS, TOP_K)

    def draw_weight(draw_key, arr_shape, std_scale):
        return (jax.random.normal(draw_key, arr_shape, jnp.float32) * std_scale).astype(jnp.bfloat16)

    return {
        'x_start': jax.random.normal(part_keys[0], tok_shape, jnp.float32).astype(jnp.bfloat16),
        'route_a': draw_routing(part_keys[1]),
        'route_b': draw_routing(part_keys[2]),
        'gate_a': jax.random.uniform(part_keys[3], pair_shape, jnp.float32, 0.5, 1.5) * gate_scale,
        'gate_b': jax.random.uniform(part_keys[4], pair_shape, jnp.float32, 0.5, 1.5) * gate_scale,
        'grad_out': jax.random.normal(part_keys[5], tok_shape, jnp.float32).astype(jnp.bfloat16),
        'w1_a': draw_weight(weight_keys[0], up_shape, up_scale),
        'w3_a': draw_weight(weight_keys[1], up_shape, up_scale),
        'w2_a': draw_weight(weight_keys[2], down_shape, down_scale),
        'w1_b': draw_weight(weight_keys[3], up_shape, up_scale),
        'w3_b': draw_weight(weight_keys[4], up_shape, up_scale),
        'w2_b': draw_weight(weight_keys[5], down_shape, down_scale),
    }


def pair_rows(route_ids):
    per_dev = route_ids.reshape(PART_DEVS, TOKENS_DEV * TOP_K)
    expert_range = jnp.arange(EXPERTS, dtype=jnp.int32)

    def dev_slots(dev_ids):
        onehot = (dev_ids[:, None] == expert_range[None, :]).astype(jnp.int32)
        earlier = jnp.cumsum(onehot, axis=0) - onehot
        return jnp.sum(earlier * onehot, axis=1)

    slot_ids = lax.map(dev_slots, per_dev)
    dev_index = jnp.arange(PART_DEVS, dtype=jnp.int32)[:, None]
    return (per_dev * SLOT_ROWS + dev_index * CAPACITY + slot_ids).reshape(-1)


def to_buffer(pair_vals, pair_row):
    filled = jnp.zeros((EXPERTS * SLOT_ROWS,) + pair_vals.shape[1:], pair_vals.dtype).at[pair_row].set(pair_vals)
    return filled.reshape((EXPERTS, SLOT_ROWS) + pair_vals.shape[1:])


def from_buffer(filled, pair_row):
    flat_rows = filled.reshape((EXPERTS * SLOT_ROWS,) + filled.shape[2:])
    picked = flat_rows[pair_row]
    return picked.reshape((PART_TOKENS, TOP_K) + filled.shape[2:])


def expert_fwd(operands):
    tok_rows, w_up1, w_up3, w_down = operands
    pre_one = jnp.dot(tok_rows, w_up1, preferred_element_type=jnp.float32)
    pre_three = jnp.dot(tok_rows, w_up3, preferred_element_type=jnp.float32)
    hidden = (jax.nn.silu(pre_one) * pre_three).astype(jnp.bfloat16)
    return jnp.dot(hidden, w_down, preferred_element_type=jnp.float32).astype(jnp.bfloat16)


def expert_bwd(operands):
    tok_rows, grad_rows, gate_rows, w_up1, w_up3, w_down = operands
    pre_one = jnp.dot(tok_rows, w_up1, preferred_element_type=jnp.float32)
    pre_three = jnp.dot(tok_rows, w_up3, preferred_element_type=jnp.float32)
    sig_one = jax.nn.sigmoid(pre_one)
    act_one = pre_one * sig_one
    hidden = (act_one * pre_three).astype(jnp.bfloat16)
    back_proj = jnp.dot(grad_rows, w_down.T, preferred_element_type=jnp.float32)
    gate_grad = jnp.sum(back_proj * hidden.astype(jnp.float32), axis=1)
    scaled_dy = (gate_rows[:, None] * grad_rows.astype(jnp.float32)).astype(jnp.bfloat16)
    dw_down = jnp.dot(hidden.T, scaled_dy, preferred_element_type=jnp.float32)
    d_hidden = gate_rows[:, None] * back_proj
    d_pre_one = (d_hidden * pre_three * sig_one * (1.0 + pre_one * (1.0 - sig_one))).astype(jnp.bfloat16)
    d_pre_three = (d_hidden * act_one).astype(jnp.bfloat16)
    dw_up1 = jnp.dot(tok_rows.T, d_pre_one, preferred_element_type=jnp.float32)
    dw_up3 = jnp.dot(tok_rows.T, d_pre_three, preferred_element_type=jnp.float32)
    grad_in = (jnp.dot(d_pre_one, w_up1.T, preferred_element_type=jnp.float32)
               + jnp.dot(d_pre_three, w_up3.T, preferred_element_type=jnp.float32)).astype(jnp.bfloat16)
    return grad_in, gate_grad, dw_up1, dw_up3, dw_down


def layer_fwd(x_in, pair_row, gate_vals, w_up1, w_up3, w_down):
    tok_rows = to_buffer(jnp.repeat(x_in, TOP_K, axis=0), pair_row)
    out_rows = lax.map(expert_fwd, (tok_rows, w_up1, w_up3, w_down))
    pair_out = from_buffer(out_rows, pair_row).astype(jnp.float32)
    mixed_sum = jnp.sum(gate_vals[:, :, None] * pair_out, axis=1)
    return (x_in.astype(jnp.float32) + mixed_sum).astype(jnp.bfloat16)


def layer_bwd(x_in, pair_row, gate_vals, w_up1, w_up3, w_down, grad_in):
    tok_rows = to_buffer(jnp.repeat(x_in, TOP_K, axis=0), pair_row)
    grad_rows = to_buffer(jnp.repeat(grad_in, TOP_K, axis=0), pair_row)
    gate_rows = to_buffer(gate_vals.reshape(-1), pair_row)
    du_rows, gate_grad, dw_up1, dw_up3, dw_down = lax.map(expert_bwd, (tok_rows, grad_rows, gate_rows, w_up1, w_up3, w_down))
    pair_grad = from_buffer(du_rows, pair_row).astype(jnp.float32)
    grad_x = (grad_in.astype(jnp.float32) + jnp.sum(pair_grad, axis=1)).astype(jnp.bfloat16)
    return grad_x, dw_up1, dw_up3, dw_down, from_buffer(gate_grad, pair_row)


def reference(x_start, route_a, route_b, gate_a, gate_b, grad_out, w1_a, w3_a, w2_a, w1_b, w3_b, w2_b):
    rows_a = pair_rows(route_a)
    rows_b = pair_rows(route_b)
    x_mid = layer_fwd(x_start, rows_a, gate_a, w1_a, w3_a, w2_a)
    x_final = layer_fwd(x_mid, rows_b, gate_b, w1_b, w3_b, w2_b)
    grad_mid, dw1_b, dw3_b, dw2_b, dgate_b = layer_bwd(x_mid, rows_b, gate_b, w1_b, w3_b, w2_b, grad_out)
    grad_x, dw1_a, dw3_a, dw2_a, dgate_a = layer_bwd(x_start, rows_a, gate_a, w1_a, w3_a, w2_a, grad_mid)
    return (x_final, grad_x, dw1_a, dw3_a, dw2_a, dw1_b, dw3_b, dw2_b, dgate_a, dgate_b)
```

```python
import jax
import jax.numpy as jnp
from jax import lax
from jax.sharding import PartitionSpec as P


F32 = jnp.float32
BF16 = jnp.bfloat16


def pair_slots(expert_ids, n_experts):
    n_tokens = expert_ids.shape[0]
    experts = jnp.arange(n_experts, dtype=jnp.int32)
    hit = expert_ids[:, :, None] == experts[None, None, :]
    count = jnp.any(hit, axis=1).astype(BF16)
    rows = lax.broadcasted_iota(jnp.int32, (n_tokens, n_tokens), 0)
    cols = lax.broadcasted_iota(jnp.int32, (n_tokens, n_tokens), 1)
    below = (cols < rows).astype(BF16)
    earlier = jnp.dot(below, count, preferred_element_type=F32).astype(jnp.int32)
    slot = jnp.sum(jnp.where(hit, earlier[:, None, :], 0), axis=2)
    return slot


def local_codes(expert_ids, slot, n_local, capacity, which):
    code = (expert_ids // n_local) * capacity + slot
    return jnp.where(expert_ids % n_local == which, code, -1)


def row_picker(code, n_rows):
    ids = lax.broadcasted_iota(jnp.int32, (n_rows, code.shape[0]), 0)
    picked = code[:, 0][None, :] == ids
    for j in range(1, code.shape[1]):
        picked = picked | (code[:, j][None, :] == ids)
    return picked.astype(BF16)


def token_picker(code_col, n_rows):
    ids = lax.broadcasted_iota(jnp.int32, (code_col.shape[0], n_rows), 1)
    return code_col[:, None] == ids


def place_gates(gate_vals, code, n_rows):
    ids = lax.broadcasted_iota(jnp.int32, (code.shape[0], n_rows), 1)
    total = jnp.zeros((code.shape[0], n_rows), F32)
    for j in range(code.shape[1]):
        total = total + jnp.where(code[:, j][:, None] == ids, gate_vals[:, j][:, None], 0.0)
    return jnp.sum(total, axis=0)


def solution(mesh):
    n_ep = mesh.shape['ep']
    n_dp = mesh.shape['dp']
    tok_spec = P(('pod', 'dp', 'ep'), None)
    weight_spec = P('ep', None, None)
    grad_spec = P(('pod', 'ep'), 'dp', None)
    assert n_dp == 2

    def local_step(x_start, route_a, route_b, gate_a, gate_b, grad_out, w1_a, w3_a, w2_a, w1_b, w3_b, w2_b):
        n_tokens, _ = x_start.shape
        top_k = route_a.shape[1]
        n_local, _, _ = w1_a.shape
        n_experts = n_local * n_ep
        capacity = 3 * n_tokens * top_k // (2 * n_experts)
        n_rows = n_ep * capacity
        dp = lax.axis_index('dp')

        def exchange(rows):
            shaped = rows.reshape((n_ep, capacity) + rows.shape[1:])
            return lax.all_to_all(shaped, 'ep', 0, 0).reshape(rows.shape)

        def dispatch(values, code):
            return jnp.dot(row_picker(code, n_rows), values, preferred_element_type=F32).astype(BF16)

        def plan(expert_ids):
            slot = pair_slots(expert_ids, n_experts)
            codes = [local_codes(expert_ids, slot, n_local, capacity, i) for i in range(n_local)]
            return codes, expert_ids * capacity + slot

        def expert_forward(rows, w_up1, w_up3, w_down):
            pre_one = jnp.dot(rows, w_up1, preferred_element_type=F32)
            pre_three = jnp.dot(rows, w_up3, preferred_element_type=F32)
            hidden = (jax.nn.silu(pre_one) * pre_three).astype(BF16)
            return jnp.dot(hidden, w_down, preferred_element_type=F32).astype(BF16)

        def mix_back(x_in, returned, codes, gate_vals):
            total = x_in.astype(F32)
            for rows, code in zip(returned, codes):
                for j in range(top_k):
                    picker = token_picker(code[:, j], n_rows).astype(BF16)
                    picked = jnp.dot(picker, rows, preferred_element_type=F32)
                    total = total + gate_vals[:, j][:, None] * picked
            return total.astype(BF16)

        def add_back(grad_in, returned, codes):
            total = grad_in.astype(F32)
            for i, code in enumerate(codes):
                picker = token_picker(code[:, 0], n_rows)
                for j in range(1, top_k):
                    picker = picker | token_picker(code[:, j], n_rows)
                total = total + jnp.dot(picker.astype(BF16), returned[i], preferred_element_type=F32)
            return total.astype(BF16)

        def gates_out(gate_vals, pair_row):
            placed = lax.optimization_barrier(place_gates(gate_vals, pair_row, n_experts * capacity))
            moved = lax.all_to_all(placed.reshape(n_ep, n_local * capacity), 'ep', 0, 0)
            moved = moved.reshape(n_ep, n_local, capacity)
            return [moved[:, i].reshape(n_rows) for i in range(n_local)]

        def gates_back(gate_grads, pair_row):
            joined = jnp.stack([grad.reshape(n_ep, capacity) for grad in gate_grads], axis=1)
            moved = lax.all_to_all(joined.reshape(n_ep, n_local * capacity), 'ep', 0, 0).reshape(-1)
            moved, pair_row = lax.optimization_barrier((moved, pair_row))
            cols = [jnp.sum(jnp.where(token_picker(pair_row[:, j], n_experts * capacity), moved[None, :], 0.0), axis=1)
                    for j in range(top_k)]
            return jnp.stack(cols, axis=1)

        def part(values, index):
            size = values.shape[1] // n_dp
            return lax.dynamic_slice_in_dim(values, index * size, size, axis=1)

        def grad_product(left, right):
            return lax.dot_general(left, right, (((0,), (0,)), ((), ())), preferred_element_type=F32)

        def to_peer(left, right):
            partial = grad_product(part(left, 1 - dp), right).astype(BF16)
            return lax.ppermute(partial, 'dp', [(0, 1), (1, 0)])

        def own_parts(lefts, rights, received):
            out = jnp.zeros((n_local, lefts[0].shape[1] // n_dp, rights[0].shape[1]), F32)
            for i in range(n_local):
                total = grad_product(part(lefts[i], dp), rights[i]) + received[i].astype(F32)
                out = lax.dynamic_update_slice(out, total[None], (i, 0, 0))
            return out

        def recompute(rows, w_up1, w_up3):
            pre_one = jnp.dot(rows, w_up1, preferred_element_type=F32)
            pre_three = jnp.dot(rows, w_up3, preferred_element_type=F32)
            hidden = (jax.nn.silu(pre_one) * pre_three).astype(BF16)
            return pre_one, pre_three, hidden

        def backward_inner(pre_one, pre_three, hidden, recv_dy, recv_gate, w_down):
            sig_one = jax.nn.sigmoid(pre_one)
            act_one = pre_one * sig_one
            back_proj = jnp.einsum('rd,fd->rf', recv_dy, w_down, preferred_element_type=F32)
            gate_grad = jnp.sum(back_proj * hidden.astype(F32), axis=-1)
            d_hidden = recv_gate[:, None] * back_proj
            d_one = (d_hidden * pre_three * sig_one * (1.0 + pre_one * (1.0 - sig_one))).astype(BF16)
            d_three = (d_hidden * act_one).astype(BF16)
            return gate_grad, d_one, d_three

        def row_grads(d_one, d_three, w_up1, w_up3):
            return (jnp.einsum('rf,df->rd', d_one, w_up1, preferred_element_type=F32)
                    + jnp.einsum('rf,df->rd', d_three, w_up3, preferred_element_type=F32)).astype(BF16)

        every = range(n_local)

        codes_a, pair_a = plan(route_a)
        codes_b, pair_b = plan(route_b)

        recv_a = [exchange(dispatch(x_start, codes_a[i])) for i in every]
        back_a = []
        for i in every:
            out_rows = expert_forward(recv_a[i], w1_a[i], w3_a[i], w2_a[i])
            back_a.append(exchange(out_rows))
        x_mid = mix_back(x_start, back_a, codes_a, gate_a)
        recv_b = [exchange(dispatch(x_mid, codes_b[i])) for i in every]

        x_kept, grad_kept = lax.optimization_barrier((x_start, grad_out))
        rows_b = [lax.optimization_barrier(rows) for rows in recv_b]

        def back_up(rows, grad_in, codes, pair_row, gate_vals, w_up1, w_up3, w_down):
            dy = [exchange(dispatch(grad_in, codes[i])) for i in every]
            gates = gates_out(gate_vals, pair_row)
            hid, pre, scaled, got2, gate_grads, d_one, d_three = [], [], [], [], [], [], []
            for i in every:
                one, three, hidden = recompute(rows[i], w_up1[i], w_up3[i])
                scaled.append((gates[i][:, None] * dy[i].astype(F32)).astype(BF16))
                one, three, hidden = lax.optimization_barrier((one, three, hidden))
                got2.append(to_peer(hidden, scaled[i]))
                hid.append(hidden)
                pre.append((one, three))
            for i in every:
                grad, one, three = backward_inner(pre[i][0], pre[i][1], hid[i], dy[i], gates[i], w_down[i])
                gate_grads.append(grad)
                d_one.append(one)
                d_three.append(three)
            got1 = [to_peer(rows[i], d_one[i]) for i in every]
            got3 = [to_peer(rows[i], d_three[i]) for i in every]
            returned = []
            for i in every:
                du_rows = row_grads(d_one[i], d_three[i], w_up1[i], w_up3[i])
                returned.append(exchange(du_rows))
            grad_x = add_back(grad_in, returned, codes)
            gate_out = gates_back(gate_grads, pair_row)

            def own():
                return (own_parts(rows, d_one, got1), own_parts(rows, d_three, got3),
                        own_parts(hid, scaled, got2))

            return grad_x, gate_out, own

        grad_mid, dgate_b, own_b = back_up(rows_b, grad_kept, codes_b, pair_b, gate_b, w1_b, w3_b, w2_b)
        rows_a = [exchange(dispatch(x_kept, codes_a[i])) for i in every]
        grad_x, dgate_a, own_a = back_up(rows_a, grad_mid, codes_a, pair_a, gate_a, w1_a, w3_a, w2_a)

        back_b = []
        for i in every:
            out_rows = expert_forward(recv_b[i], w1_b[i], w3_b[i], w2_b[i])
            back_b.append(exchange(out_rows))
        x_final = mix_back(x_mid, back_b, codes_b, gate_b)

        dw1_b, dw3_b, dw2_b = own_b()
        dw1_a, dw3_a, dw2_a = own_a()
        return (x_final, grad_x, dw1_a, dw3_a, dw2_a, dw1_b, dw3_b, dw2_b, dgate_a, dgate_b)

    return jax.shard_map(local_step, mesh=mesh,
                         in_specs=(tok_spec,) * 6 + (weight_spec,) * 6,
                         out_specs=(tok_spec, tok_spec) + (grad_spec,) * 6 + (tok_spec, tok_spec),
                         check_vma=False)
```
